32 devices in a mesh: dp: 4 (over y, core), mp: 2 (over x), section: 4 (over z).
Axes of the slice: x: 2, y: 2, z: 4, core: 2. Of those that a mesh axis runs over, the one named last changes fastest.
Arguments:
- hidden_in: bfloat16 [64, 2560], P('dp', 'mp'), may hold values from -6 to 6
- lengths: int32 [64], P('dp'), may hold values from 0 to 7
- slots: int32 [64], P('dp'), may hold values from 0 to 71, as said below
- norm_gain: float32 [4, 2560], P('section'), may hold values from 0.5 to 1.5
- w_zxo: bfloat16 [4, 3, 5120, 2560], P('section', None, 'dp', 'mp'), may hold values from -0.125 to 0.125
- w_bcdt: bfloat16 [4, 336, 2560], P('section', 'dp', 'mp'), may hold values from -0.125 to 0.125
- conv_x_weight: float32 [4, 4, 5120], P('section', None, 'mp'), may hold values from -0.5 to 0.5
- conv_bc_weight: float32 [4, 4, 256], P('section'), may hold values from -0.5 to 0.5
- conv_x_pool: bfloat16 [4, 72, 3, 5120], P('section', 'dp', None, 'mp'), may hold values from -6 to 6
- conv_bc_pool: bfloat16 [4, 72, 3, 256], P('section', 'dp'), may hold values from -6 to 6
- state_pool: float32 [4, 72, 80, 64, 128], P('section', 'dp', 'mp'), may hold values from -1 to 1
- a_rate: float32 [4, 80], P('section', 'mp'), may hold values from 1 to 16
- dt_bias: float32 [4, 80], P('section', 'mp'), may hold values from -3 to 0
- skip_gain: float32 [4, 80], P('section', 'mp'), may hold values from 0.5 to 1.5
- gate_gain: float32 [4, 5120], P('section', 'mp'), may hold values from 0.5 to 1.5
Outputs:
- hidden_out: bfloat16 [4, 64, 2560], P('section', 'dp', 'mp')
- state_out: float32 [4, 64, 80, 64, 128], P('section', 'dp', 'mp')
The draws below stay inside these ranges and needn't reach their ends.
Inputs may be any that keep to these rules, and one draw needn't show every extreme that they name: The sequences of the d-th block of 16 name distinct slots, all from d * 18 to (d + 1) * 18 - 1.
All inputs are finite; a program needn't handle non-finite values.
Results may differ from the reference program's by a relative error of at most 0.025.
Values may be sent and summed in bfloat16 or wider, within the bound.
No kernel may reach another device: no remote copies, remote signals or barrier semaphores. Data moves between devices by JAX's collectives and lax.ppermute only.
A program may use at most 192 MiB of HBM per device.

```python
import math
import jax
import jax.numpy as jnp
from jax import lax

D = 2560
H = 80
P_SIZE = 64
N = 128
SEQ_DEV = 16
SLOTS_DEV = 18
DI = 5120
LAYERS = 4
SEQ = 64
SLOTS = 72


def draw_slots(key, part):
    blocks = SEQ // SEQ_DEV
    block_keys = jax.random.split(key, blocks)

    def one_block(block_key, block_index):
        chosen = jax.random.permutation(block_key, SLOTS_DEV)[:SEQ_DEV].astype(jnp.int32)
        return chosen + block_index * SLOTS_DEV
    return jax.vmap(one_block)(block_keys, jnp.arange(blocks, dtype=jnp.int32)).reshape(SEQ).astype(jnp.int32)


def touch_ends(entries, stream_key, smallest, high):
    extent = entries.shape
    index_at = [jax.random.randint(jax.random.fold_in(stream_key, axis), (), 0, extent[axis]) for axis in range(len(extent))]
    entries = entries.at[tuple(index_at)].set(smallest)
    longest = extent.index(max(extent))
    index_at[longest] = (index_at[longest] + 1) % extent[longest]
    return entries.at[tuple(index_at)].set(high)


def block_levels(rng, shape, cuts, low, top_value):
    factor_of, own = 1.0, jax.random.fold_in(rng, 6)
    for dim, blocks in cuts:
        steps = jnp.exp(jax.random.uniform(jax.random.fold_in(own, dim), (blocks,), jnp.float32, low / len(cuts), top_value / len(cuts)))
        factor_of = factor_of * jnp.repeat(steps, shape[dim] // blocks).reshape([-1 if axis == dim else 1 for axis in range(len(shape))])
    return factor_of


def bell_draw(rng, shape, spread, reach, cuts=(), kind=jnp.bfloat16):
    values = jax.random.normal(rng, shape, jnp.float32) * spread
    if len(cuts) > 0:
        values = block_levels(rng, shape, cuts, -0.22, 0.18) * values
    return jnp.clip(values, min=-reach, max=reach).astype(kind)


def setup_inputs(seed: int = 0) -> dict:
    arg_keys = jax.random.split(jax.random.key(seed), 16)
    return {
        "hidden_in": bell_draw(arg_keys[0], (SEQ, D), 1.0, 6.0, ((0, 4), (1, 2))),
        "lengths": touch_ends(jax.random.randint(arg_keys[1], (SEQ,), 0, 8), jax.random.fold_in(arg_keys[1], 1), 0, 7).astype(jnp.int32),
        "slots": draw_slots(jax.random.fold_in(arg_keys[15], 71), 0),
        "norm_gain": jnp.clip(1.0 + 0.1 * jax.random.normal(arg_keys[3], (LAYERS, D), jnp.float32), 0.5, 1.5),
        "w_zxo": bell_draw(arg_keys[4], (LAYERS, 3, DI, D), D ** -0.5, 0.125, ((0, 4), (2, 4), (3, 2))),
        "w_bcdt": bell_draw(arg_keys[5], (LAYERS, 2 * N + H, D), D ** -0.5, 0.125, ((0, 4), (1, 4), (2, 2))),
        "conv_x_weight": jnp.clip(jax.random.uniform(arg_keys[6], (LAYERS, 4, DI), jnp.float32, -0.5, 0.5) * block_levels(arg_keys[6], (LAYERS, 4, DI), ((0, 4), (2, 2)), -0.4, 0.0), -0.5, 0.5),
        "conv_bc_weight": jnp.clip(jax.random.uniform(arg_keys[7], (LAYERS, 4, 2 * N), jnp.float32, -0.5, 0.5) * block_levels(arg_keys[7], (LAYERS, 4, 2 * N), ((0, 4),), -0.4, 0.0), -0.5, 0.5),
        "conv_x_pool": bell_draw(arg_keys[8], (LAYERS, SLOTS, 3, DI), 1.0, 6.0, ((0, 4), (1, 4), (3, 2))),
        "conv_bc_pool": bell_draw(arg_keys[9], (LAYERS, SLOTS, 3, 2 * N), 1.0, 6.0, ((0, 4), (1, 4))),
        "state_pool": bell_draw(arg_keys[10], (LAYERS, SLOTS, H, P_SIZE, N), 0.15, 1.0, ((0, 4), (1, 4), (2, 2)), jnp.float32),
        "a_rate": jnp.clip(jnp.exp(math.log(16.0) - 2.7725887 * jax.random.uniform(arg_keys[11], (LAYERS, H), jnp.float32) ** block_levels(arg_keys[11], (LAYERS, H), ((0, 4), (1, 2)), -0.2, 0.2)), 1.0, 16.0),
        "dt_bias": jnp.clip(-3.0 + 3.0 * jax.random.uniform(arg_keys[12], (LAYERS, H), jnp.float32) ** block_levels(arg_keys[12], (LAYERS, H), ((0, 4), (1, 2)), -0.2, 0.2), -3.0, 0.0),
        "skip_gain": jnp.clip(0.5 + 1.0 * jax.random.uniform(arg_keys[13], (LAYERS, H), jnp.float32) ** block_levels(arg_keys[13], (LAYERS, H), ((0, 4), (1, 2)), -0.2, 0.2), 0.5, 1.5),
        "gate_gain": jnp.clip(1.0 + 0.1 * jax.random.normal(arg_keys[14], (LAYERS, DI), jnp.float32), 0.5, 1.5),
    }


epsilon = 1e-05

def project(inputs, weights):
    return lax.dot_general(inputs, weights, (((1,), (1,)), ((), ())), preferred_element_type=jnp.float32)

def convolve(history, current, kernel, tap_mask):
    past_sum = lax.optimization_barrier(jnp.sum(history.astype(jnp.float32) * tap_mask[:, :, None] * kernel[None, :3, :], axis=1))
    return jax.nn.silu(past_sum + current * kernel[3][None, :])

def reference(hidden_in, lengths, slots, norm_gain, w_zxo, w_bcdt, conv_x_weight, conv_bc_weight, conv_x_pool, conv_bc_pool, state_pool, a_rate, dt_bias, skip_gain, gate_gain):
    tap_mask = (lengths[:, None] >= (3 - jnp.arange(3, dtype=jnp.int32))[None, :]).astype(jnp.float32)
    alive = (lengths > 0).astype(jnp.float32)
    hidden = hidden_in
    hiddens = []
    states = []
    for layer_index in range(LAYERS):
        residual = hidden.astype(jnp.float32)
        normed_in = (residual * lax.rsqrt(lax.optimization_barrier(jnp.mean(residual * residual, axis=1, keepdims=True)) + epsilon) * norm_gain[layer_index][None, :]).astype(jnp.bfloat16)
        gate_proj = project(normed_in, w_zxo[layer_index, 0])
        inner_proj = project(normed_in, w_zxo[layer_index, 1])
        small_proj = project(normed_in, w_bcdt[layer_index])
        step_raw = small_proj[:, 2 * N:]
        conv_x = convolve(jnp.take(conv_x_pool[layer_index], slots, axis=0), inner_proj, conv_x_weight[layer_index], tap_mask)
        conv_bc = convolve(jnp.take(conv_bc_pool[layer_index], slots, axis=0), small_proj[:, :2 * N], conv_bc_weight[layer_index], tap_mask)
        conv_b = conv_bc[:, :N]
        conv_c = conv_bc[:, N:]
        step_size = jax.nn.softplus(step_raw + dt_bias[layer_index][None, :])
        decay_rate = jnp.exp(-step_size * a_rate[layer_index][None, :])
        old_state = jnp.take(state_pool[layer_index], slots, axis=0) * alive[:, None, None, None]
        inner_heads = conv_x.reshape(SEQ, H, P_SIZE)
        new_state = decay_rate[:, :, None, None] * old_state + (step_size[:, :, None] * inner_heads)[:, :, :, None] * conv_b[:, None, None, :]
        read_out = jnp.einsum('bhpn,bn->bhp', new_state, conv_c, precision=lax.Precision.HIGHEST) + skip_gain[layer_index][None, :, None] * inner_heads
        gated = read_out.reshape(SEQ, H * P_SIZE) * jax.nn.silu(gate_proj)
        normed = (gated * lax.rsqrt(lax.optimization_barrier(jnp.mean(gated * gated, axis=1, keepdims=True)) + epsilon) * gate_gain[layer_index][None, :]).astype(jnp.bfloat16)
        summed = jnp.dot(normed, w_zxo[layer_index, 2], preferred_element_type=jnp.float32)
        hidden = (residual + summed).astype(jnp.bfloat16)
        hiddens.append(hidden)
        states.append(new_state)
    return (jnp.stack(hiddens), jnp.stack(states))
```

```python
import functools

import jax
import jax.numpy as jnp
from jax import lax
from jax.experimental import pallas as pl
from jax.experimental.pallas import tpu as pltpu
from jax.sharding import PartitionSpec as P

epsilon = 1e-05
LANES = 128
SUBLANES = 8
MEBI = 1 << 20
CHUNKS = 4


def padded(width):
    return -(-width // LANES) * LANES


def in_vmem(count):
    return [pl.BlockSpec(memory_space=pltpu.VMEM)] * count


def in_smem(count):
    return [pl.BlockSpec(memory_space=pltpu.SMEM)] * count


def lanes_of(shape):
    return lax.broadcasted_iota(jnp.int32, shape, 1)


def two_parts(column, lane):
    high = column.astype(jnp.bfloat16).astype(jnp.float32)
    low = column - high
    return jnp.where(lane == 0, high, jnp.where(lane == 1, low, 0.0))


def against(inputs, weights):
    return lax.dot_general(
        inputs, weights, (((1,), (1,)), ((), ())), preferred_element_type=jnp.float32
    )


def load_kernel(
    pieces,
    slots_ref,
    lengths_ref,
    pool_ref,
    w_ref,
    conv_x_ref,
    conv_bc_ref,
    table_ref,
    heads_ref,
    *refs,
):
    held_refs = refs[:CHUNKS]
    (
    w_out_ref,
    past_x_ref,
    past_bc_ref,
    wide_ref,
    head_ref,
    now_bc_ref,
    alive_ref,
    history_x,
    history_bc,
    sems,
    w_sems,
    small_sems,
    ) = refs[CHUNKS:]
    chunk, heads = held_refs[0].shape[:2]
    rows = chunk * CHUNKS
    chan = past_x_ref.shape[1]
    each = heads // pieces

    def copies(c, i):
        for k in range(pieces):
            part = pl.ds(k * each, each)
            yield pltpu.make_async_copy(
                pool_ref.at[0, slots_ref[c * chunk + i], part],
                held_refs[c].at[i, part],
                sems.at[c * chunk + i, k],
            )

    small_copies = [
        pltpu.make_async_copy(source, target, small_sems.at[k])
        for k, (source, target) in enumerate(
            (
                (conv_x_ref, history_x),
                (conv_bc_ref, history_bc),
            )
        )
    ]
    w_copies = [
        pltpu.make_async_copy(w_ref.at[0, k], w_out_ref.at[k], w_sems.at[k])
        for k in range(w_out_ref.shape[0])
    ]
    for copy in small_copies + w_copies:
        copy.start()

    for c in range(CHUNKS):

        def start(i, carry):
            for copy in copies(c, i):
                copy.start()
            return carry

        lax.fori_loop(0, chunk, start, 0)
    for copy in small_copies:
        copy.wait()
    alive = jnp.zeros(alive_ref.shape, jnp.float32)
    row = lax.broadcasted_iota(jnp.int32, alive_ref.shape, 0)
    for i in range(rows):
        length = lengths_ref[i]
        for history_ref, above, past_ref in (
            (history_x, 0, past_x_ref),
            (history_bc, 4, past_bc_ref),
        ):
            history = history_ref[0, slots_ref[i]].astype(jnp.float32)
            taps = history.shape[0]
            tap = lax.broadcasted_iota(jnp.int32, (taps, 1), 0)
            known = (length >= taps - tap).astype(jnp.float32)
            past_ref[i : i + 1, :] = jnp.sum(
                history * known * table_ref[above : above + taps, : history.shape[1]],
                axis=0, keepdims=True
            )
        alive = jnp.where(row == i, (length > 0).astype(jnp.float32), alive)
    alive_ref[...] = alive
    onto = lax.broadcasted_iota(jnp.int32, (heads, chan), 0)
    onto = (onto == lanes_of((heads, chan)) // (chan // heads)).astype(jnp.float32)
    for k in range(3):
        wide = jnp.dot(
            jnp.broadcast_to(heads_ref[k : k + 1, :], (SUBLANES, heads)),
            onto,
            precision=lax.Precision.HIGHEST,
            preferred_element_type=jnp.float32,
        )
        wide_ref[k : k + 1, :] = wide[:1]
    wide_ref[3:4, :] = table_ref[8:9, :]
    wide_ref[4:5, :] = table_ref[3:4, :]
    now_bc_ref[...] = table_ref[7:8, : now_bc_ref.shape[1]]
    head_ref[...] = heads_ref[:2, :]
    for copy in w_copies:
        copy.wait()
    for c in range(CHUNKS):

        def wait(i, carry):
            for copy in copies(c, i):
                copy.wait()
            return carry

        lax.fori_loop(0, chunk, wait, 0)


def load(slots, lengths, pool, w, conv_x, conv_bc, table, by_head):
    rows = slots.shape[0]
    heads, head_size, width = pool.shape[2:]
    pieces = 2 if heads % 2 == 0 else 1
    chan = conv_x.shape[3]
    bc_width = conv_bc.shape[3]
    made = rows * heads * head_size * width * 4 + w.size * 2
    return pl.pallas_call(
        functools.partial(load_kernel, pieces),
        out_shape=[
            *[jax.ShapeDtypeStruct((rows // CHUNKS, heads, head_size, width), jnp.float32)] * CHUNKS,
            jax.ShapeDtypeStruct(w.shape[1:], jnp.bfloat16),
            jax.ShapeDtypeStruct((rows, chan), jnp.float32),
            jax.ShapeDtypeStruct((rows, bc_width), jnp.float32),
            jax.ShapeDtypeStruct((5, chan), jnp.float32),
            jax.ShapeDtypeStruct((2, heads), jnp.float32),
            jax.ShapeDtypeStruct((1, bc_width), jnp.float32),
            jax.ShapeDtypeStruct((rows, LANES), jnp.float32),
        ],
        in_specs=in_smem(2) + [pl.BlockSpec(memory_space=pltpu.HBM)] * 4 + in_vmem(2),
        out_specs=in_vmem(7 + CHUNKS),
        scratch_shapes=[
            pltpu.VMEM(conv_x.shape, conv_x.dtype),
            pltpu.VMEM(conv_bc.shape, conv_bc.dtype),
            pltpu.SemaphoreType.DMA((rows, pieces)),
            pltpu.SemaphoreType.DMA((w.shape[1],)),
            pltpu.SemaphoreType.DMA((2,)),
        ],
        compiler_params=pltpu.CompilerParams(vmem_limit_bytes=5 * MEBI),
        cost_estimate=pl.CostEstimate(
            flops=rows * heads * head_size * width * 16, bytes_accessed=made, transcendentals=0
        ),
        name="load",
    )(slots, lengths, pool, w, conv_x, conv_bc, table, by_head)


def for_each_part(target, parts, act):
    if parts == 1:
        act(0)
        return
    for part in range(parts):
        pl.when(target % parts == part)(functools.partial(act, part))


def row_of(target, parts, group, seq_dev, mine):
    block = target // parts
    return pl.multiple_of((((block % group) ^ mine) * 2 + block // group) * seq_dev, seq_dev)


def project_kernel(
    parts, seq_dev, sharers, group, blocks, place_ref, gain_ref, w_ref, *refs
):
    small_refs = refs[:sharers]
    hidden_refs = refs[sharers : sharers + group]
    *out_refs, scaled_ref, held = refs[sharers + group :]
    chan = w_ref.shape[1]
    piece = chan // parts
    wide = 2 * chan
    source, dp_index = place_ref[2], place_ref[3]
    lane = lanes_of((hidden_refs[0].shape[0], LANES))
    for k, hidden_ref in enumerate(hidden_refs):
        hidden = hidden_ref[...].astype(jnp.float32)
        rows = slice(k * hidden.shape[0], (k + 1) * hidden.shape[0])
        scaled_ref[rows, :] = (hidden * gain_ref[...]).astype(jnp.bfloat16)
        square = jnp.sum(hidden * hidden, axis=1, keepdims=True)
        held[rows, held.shape[1] - LANES :] = two_parts(square, lane).astype(jnp.bfloat16)
    scaled = scaled_ref[...]
    held[:, :chan] = against(scaled, w_ref[1]).astype(jnp.bfloat16)
    held[:, chan:wide] = against(scaled, w_ref[0]).astype(jnp.bfloat16)
    small_width = held.shape[1] - LANES - wide
    tail = jnp.zeros((scaled.shape[0], small_width), jnp.float32)
    for r, small_ref in enumerate(small_refs):
        count = small_ref.shape[0]
        block = ((dp_index // blocks) ^ r) * blocks + dp_index % blocks
        onto = lax.broadcasted_iota(jnp.int32, (count, small_width), 0) + block * count
        onto = (onto == lanes_of((count, small_width))).astype(jnp.bfloat16)
        small = against(scaled, small_ref[...]).astype(jnp.bfloat16)
        tail = tail + jnp.dot(small, onto, preferred_element_type=jnp.float32)
    held[:, wide : wide + small_width] = tail.astype(jnp.bfloat16)
    for r, out_ref in enumerate(out_refs):
        target = source ^ r
        rows = pl.ds(row_of(target, parts, group, seq_dev, dp_index % group), seq_dev)

        def fill(first):
            out_ref[:, :piece] = held[rows, first : first + piece]
            out_ref[:, piece : 2 * piece] = held[rows, chan + first : chan + first + piece]

        for_each_part(target, parts, lambda part: fill(part * piece))
        out_ref[:, 2 * piece :] = held[rows, wide:]


def project(parts, rounds, seq_dev, blocks, small_width, place, gain, w, smalls, hiddens):
    chan, share = w.shape[1:]
    width = 2 * chan // parts + small_width + LANES
    rows = hiddens[0].shape[0] * len(hiddens)
    return pl.pallas_call(
        functools.partial(project_kernel, parts, seq_dev, len(smalls), len(hiddens), blocks),
        out_shape=[jax.ShapeDtypeStruct((seq_dev, width), jnp.bfloat16)] * rounds,
        in_specs=in_smem(1) + in_vmem(2 + len(smalls) + len(hiddens)),
        out_specs=in_vmem(rounds),
        scratch_shapes=[
            pltpu.VMEM((rows, share), jnp.bfloat16),
            pltpu.VMEM((rows, 2 * chan + small_width + LANES), jnp.bfloat16),
        ],
        compiler_params=pltpu.CompilerParams(vmem_limit_bytes=6 * MEBI),
        cost_estimate=pl.CostEstimate(
            flops=2 * rows * share * (2 * chan + small_width),
            bytes_accessed=2 * share * (2 * chan + small_width),
            transcendentals=0,
        ),
        name="project",
    )(place, gain, w, *smalls, *hiddens)


def mix_kernel(
    tick,
    rounds,
    parts,
    mp_count,
    model_width,
    heads,
    place_ref,
    past_x_ref,
    past_bc_ref,
    now_bc_ref,
    wide_ref,
    head_ref,
    alive_ref,
    *refs,
):
    held_refs = refs[:CHUNKS]
    refs = refs[CHUNKS:]
    got_refs = refs[:rounds]
    before_refs = refs[rounds : rounds + 3 * (tick > 0)]
    refs = refs[rounds + len(before_refs) :]
    out_refs = refs[:rounds]
    decay_ref, x_ref, b_ref, c_ref, read_ref, gated_ref, inner_ref, gate_ref = refs[rounds:]

    def keep(k, ref, value):
        if tick > 0:
            value = jnp.where(place_ref[4] == tick, value, before_refs[k][...])
        ref[...] = value

    seq_dev, chan = past_x_ref.shape
    head_size = chan // heads
    bc_width = past_bc_ref.shape[1]
    blocks = max(1, rounds // mp_count)
    piece = chan // blocks
    target = place_ref[0]
    mp_index = place_ref[1]
    tail_width = got_refs[0].shape[1] - 2 * piece

    for j in range(blocks):
        both = jnp.zeros((seq_dev, 2 * piece), jnp.float32)
        for r, got_ref in enumerate(got_refs):
            chosen = ((target ^ r) % blocks == j).astype(jnp.float32)
            both = both + chosen * got_ref[:, : 2 * piece].astype(jnp.float32)
        inner_ref[:, j * piece : (j + 1) * piece] = both[:, :piece]
        gate_ref[:, j * piece : (j + 1) * piece] = both[:, piece:]
    tail = jnp.zeros((seq_dev, tail_width), jnp.float32)
    for got_ref in got_refs:
        tail = tail + got_ref[:, 2 * piece :].astype(jnp.float32)
    square = jnp.sum(tail[:, tail_width - LANES :], axis=1, keepdims=True) / blocks
    scale = lax.rsqrt(square / model_width + epsilon)
    conv_bc = jax.nn.silu(past_bc_ref[...] + tail[:, :bc_width] * scale * now_bc_ref[...])
    conv_b = conv_bc[:, : bc_width // 2]
    conv_c = conv_bc[:, bc_width // 2 :]
    keep(2, b_ref, conv_b)
    c_ref[...] = conv_c
    read_ref[...] = jnp.zeros_like(read_ref)
    group = min(heads, 8)
    while group and (heads % group or group * head_size % LANES):
        group -= 1
    group = group or heads

    chunk = seq_dev // CHUNKS

    def work(c, at, carry):
        i = c * chunk + at
        c_rows = jnp.broadcast_to(c_ref[pl.ds(i, 1), :], (SUBLANES, conv_c.shape[1]))
        c_rows = c_rows.astype(jnp.bfloat16)
        found = []
        for first in range(0, heads, group):
            state = held_refs[c][at, first : first + group]
            state = state.reshape(group * head_size, state.shape[2]).astype(jnp.bfloat16)
            found.append(against(c_rows, state))
        tile = pl.ds(pl.multiple_of(i // SUBLANES * SUBLANES, SUBLANES), SUBLANES)
        width = group * head_size
        mine = lax.broadcasted_iota(jnp.int32, (SUBLANES, width), 0) == i % SUBLANES
        for k, y in enumerate(found):
            columns = slice(k * width, (k + 1) * width)
            read_ref[tile, columns] = jnp.where(mine, y, read_ref[tile, columns])
        return carry

    for c in range(CHUNKS):
        lax.fori_loop(0, chunk, functools.partial(work, c), 0)

    raw = tail[:, bc_width : tail_width - LANES] * scale
    raw_width = raw.shape[1]
    pick = lambda shape, per: (
        lax.broadcasted_iota(jnp.int32, shape, 0) == mp_index * heads + lanes_of(shape) // per
    ).astype(jnp.float32)
    chosen = lambda per, width: jnp.dot(
        raw,
        pick((raw_width, width), per),
        precision=lax.Precision.HIGHEST,
        preferred_element_type=jnp.float32,
    )
    softplus = lambda v: jnp.maximum(v, 0.0) + jnp.log1p(jnp.exp(-jnp.abs(v)))
    alive = alive_ref[:, :1]
    step_heads = softplus(chosen(1, heads) + head_ref[0:1, :])
    keep(0, decay_ref, jnp.exp(-step_heads * head_ref[1:2, :]) * alive)
    step = softplus(chosen(head_size, chan) + wide_ref[0:1, :])
    decay = jnp.exp(-step * wide_ref[1:2, :]) * alive
    conv_x = jax.nn.silu(past_x_ref[...] + inner_ref[...] * scale * wide_ref[4:5, :])
    x_step = conv_x * step
    keep(1, x_ref, x_step)
    cross = jnp.sum(conv_b * conv_c, axis=1, keepdims=True)
    y = decay * read_ref[...] + x_step * cross + wide_ref[2:3, :] * conv_x
    gated = y * jax.nn.silu(gate_ref[...] * scale)
    square = jnp.sum(gated * gated, axis=1, keepdims=True)
    gated_ref[...] = (gated * wide_ref[3:4, :]).astype(jnp.bfloat16)
    out_tail = two_parts(square, lanes_of((seq_dev, LANES))).astype(jnp.bfloat16)
    for r, out_ref in enumerate(out_refs):
        first = pl.multiple_of((target ^ r) % blocks * piece, LANES) if blocks > 1 else 0
        out_ref[:, :piece] = gated_ref[:, pl.ds(first, piece)]
        out_ref[:, piece:] = out_tail


def mix(
    tick, parts, mp_count, model_width, place, past_x, past_bc, now_bc, wide, head, alive, held,
    got, before,
):
    rounds = len(got)
    seq_dev, chan = past_x.shape
    heads = head.shape[1]
    piece = chan // max(1, rounds // mp_count)
    state_size = held[0].shape[3]
    return pl.pallas_call(
        functools.partial(mix_kernel, tick, rounds, parts, mp_count, model_width, heads),
        out_shape=[jax.ShapeDtypeStruct((seq_dev, piece + LANES), jnp.bfloat16)] * rounds
        + [
            jax.ShapeDtypeStruct((seq_dev, heads), jnp.float32),
            jax.ShapeDtypeStruct((seq_dev, chan), jnp.float32),
            jax.ShapeDtypeStruct((seq_dev, state_size), jnp.float32),
        ],
        in_specs=in_smem(1) + in_vmem(6 + CHUNKS + rounds + len(before)),
        out_specs=in_vmem(rounds + 3),
        scratch_shapes=[
            pltpu.VMEM((seq_dev, state_size), jnp.float32),
            pltpu.VMEM((seq_dev, chan), jnp.float32),
            pltpu.VMEM((seq_dev, chan), jnp.bfloat16),
            pltpu.VMEM((seq_dev, chan), jnp.float32),
            pltpu.VMEM((seq_dev, chan), jnp.float32),
        ],
        compiler_params=pltpu.CompilerParams(vmem_limit_bytes=10 * MEBI),
        cost_estimate=pl.CostEstimate(
            flops=16 * seq_dev * chan * state_size,
            bytes_accessed=seq_dev * chan * state_size * 4,
            transcendentals=0,
        ),
        name="mix",
    )(place, past_x, past_bc, now_bc, wide, head, alive, *held, *got, *before)


def finish_kernel(rounds, parts, seq_dev, group, place_ref, w_ref, *refs):
    got_refs = refs[:rounds]
    out_refs = refs[rounds : rounds + group]
    rows_ref, square_ref = refs[rounds + group :]
    piece = got_refs[0].shape[1] - LANES
    square_ref[...] = jnp.zeros_like(square_ref)
    for r, got_ref in enumerate(got_refs):
        target = place_ref[2] ^ r
        rows = pl.ds(row_of(target, parts, group, seq_dev, place_ref[3] % group), seq_dev)

        def fill(first):
            rows_ref[rows, first : first + piece] = got_ref[:, :piece]

        for_each_part(target, parts, lambda part: fill(part * piece))
        square_ref[rows, :] += got_ref[:, piece:].astype(jnp.float32)
    square = jnp.sum(square_ref[...], axis=1, keepdims=True)
    tail = two_parts(square, lanes_of(square_ref.shape)).astype(jnp.bfloat16)
    partial = jnp.dot(rows_ref[...], w_ref[2], preferred_element_type=jnp.float32)
    partial = partial.astype(jnp.bfloat16)
    for k, out_ref in enumerate(out_refs):
        rows = slice(2 * seq_dev * k, 2 * seq_dev * (k + 1))
        out_ref[:, :LANES] = tail[rows]
        out_ref[:, LANES:] = partial[rows]


def finish(parts, group, place, w, got):
    rounds = len(got)
    chan, share = w.shape[1:]
    seq_dev = got[0].shape[0]
    seq_all = 2 * seq_dev * group
    return pl.pallas_call(
        functools.partial(finish_kernel, rounds, parts, seq_dev, group),
        out_shape=[jax.ShapeDtypeStruct((2 * seq_dev, LANES + share), jnp.bfloat16)] * group,
        in_specs=in_smem(1) + in_vmem(1 + rounds),
        out_specs=in_vmem(group),
        scratch_shapes=[
            pltpu.VMEM((seq_all, chan), jnp.bfloat16),
            pltpu.VMEM((seq_all, LANES), jnp.float32),
        ],
        compiler_params=pltpu.CompilerParams(vmem_limit_bytes=6 * MEBI),
        cost_estimate=pl.CostEstimate(
            flops=2 * seq_all * chan * share, bytes_accessed=2 * chan * share, transcendentals=0
        ),
        name="finish",
    )(place, w, *got)


def settle_kernel(tick, seq_dev, group, blocks, chan_total, place_ref, mine_ref, met_ref, old_ref, *refs):
    *before_refs, hidden_ref, own_ref = refs
    total = mine_ref[...].astype(jnp.float32) + met_ref[...].astype(jnp.float32)
    square = jnp.sum(total[:, :LANES], axis=1, keepdims=True) / blocks
    scale = lax.rsqrt(square / chan_total + epsilon)
    hidden = old_ref[...].astype(jnp.float32) + total[:, LANES:] * scale
    hidden_ref[...] = hidden.astype(jnp.bfloat16)
    first = pl.multiple_of(place_ref[3] // group * seq_dev, seq_dev)
    own = hidden_ref[pl.ds(first, seq_dev), :]
    for before_ref in before_refs:
        own = jnp.where(place_ref[4] == tick, own, before_ref[...])
    own_ref[...] = own


def settle(tick, group, blocks, chan_total, place, mine, met, old, before):
    rows, share = old.shape
    return pl.pallas_call(
        functools.partial(settle_kernel, tick, rows // 2, group, blocks, chan_total),
        out_shape=[
            jax.ShapeDtypeStruct((rows, share), jnp.bfloat16),
            jax.ShapeDtypeStruct((rows // 2, share), jnp.bfloat16),
        ],
        in_specs=in_smem(1) + in_vmem(3 + len(before)),
        out_specs=in_vmem(2),
        compiler_params=pltpu.CompilerParams(vmem_limit_bytes=4 * MEBI),
        cost_estimate=pl.CostEstimate(flops=rows * share * 8, bytes_accessed=rows * share * 10, transcendentals=0),
        name="settle",
    )(place, mine, met, old, *before)


def write_kernel(decay_ref, x_ref, b_ref, *refs):
    states_refs = refs[:CHUNKS]
    out_ref, held, sems = refs[CHUNKS:]
    rows, heads, head_size, width = held.shape
    together = LANES // head_size

    def copy_out(i):
        return pltpu.make_async_copy(held.at[i], out_ref.at[0, i], sems.at[i])

    chunk = rows // CHUNKS

    def work(c, at, carry):
        i = c * chunk + at
        b_rows = jnp.broadcast_to(b_ref[pl.ds(i, 1), :], (LANES, width))
        tile = pl.ds(pl.multiple_of(i // SUBLANES * SUBLANES, SUBLANES), SUBLANES)
        for first in range(0, heads, together):
            count = min(together, heads - first)
            columns = slice(first * head_size, (first + count) * head_size)
            chosen = lax.broadcasted_iota(jnp.int32, (SUBLANES, count * head_size), 0) == i % SUBLANES
            x_row = jnp.sum(jnp.where(chosen, x_ref[tile, columns], 0.0), axis=0, keepdims=True)
            x_rows = jnp.broadcast_to(x_row, (LANES, count * head_size))
            added = x_rows.T * b_rows[: count * head_size]
            for k in range(count):
                held[i, first + k] = (
                    states_refs[c][at, first + k] * decay_ref[i, first + k]
                    + added[k * head_size : (k + 1) * head_size]
                )
        copy_out(i).start()
        return carry

    def end(i, carry):
        copy_out(i).wait()
        return carry

    for c in range(CHUNKS):
        lax.fori_loop(0, chunk, functools.partial(work, c), 0)
    lax.fori_loop(0, rows, end, 0)


def write_states(decay, x, b, states):
    chunk, heads, head_size, width = states[0].shape
    rows = chunk * len(states)
    return pl.pallas_call(
        write_kernel,
        out_shape=jax.ShapeDtypeStruct((1, rows, heads, head_size, width), jnp.float32),
        in_specs=in_smem(1) + in_vmem(2 + CHUNKS),
        out_specs=pl.BlockSpec(memory_space=pl.ANY),
        scratch_shapes=[
            pltpu.VMEM((rows, heads, head_size, width), jnp.float32),
            pltpu.SemaphoreType.DMA((rows,)),
        ],
        compiler_params=pltpu.CompilerParams(
            vmem_limit_bytes=rows * heads * head_size * width * 4 + 3 * MEBI
        ),
        cost_estimate=pl.CostEstimate(
            flops=16 * rows * heads * head_size * width,
            bytes_accessed=rows * heads * head_size * width * 8,
            transcendentals=0,
        ),
        name="write_states",
    )(decay, x, b, *states)


def local(
    hidden_in,
    lengths,
    slots,
    norm_gain,
    w_zxo,
    w_bcdt,
    conv_x_weight,
    conv_bc_weight,
    conv_x_pool,
    conv_bc_pool,
    state_pool,
    a_rate,
    dt_bias,
    skip_gain,
    gate_gain,
):
    section_index = lax.axis_index("section")
    section_count = lax.axis_size("section")
    mp_index = lax.axis_index("mp")
    mp_count = lax.axis_size("mp")
    dp_index = lax.axis_index("dp")
    dp_count = lax.axis_size("dp")
    seq_dev, model_share = hidden_in.shape
    seq_all = seq_dev * dp_count
    model_width = norm_gain.shape[1]
    heads_dev = a_rate.shape[1]
    head_size = state_pool.shape[3]
    chan_dev = heads_dev * head_size
    slots_dev = state_pool.shape[1]
    bc_width = conv_bc_weight.shape[2]
    small_dev = w_bcdt.shape[1]
    small_all = small_dev * dp_count
    chan_saved = w_zxo.shape[2]
    chan_total = chan_saved * dp_count
    small_pad = bc_width + padded(small_all - bc_width)

    blocks = max(1, dp_count // mp_count)
    parts = max(1, mp_count // dp_count)
    rounds = dp_count * parts

    def places():
        for d in range(dp_count):
            for m in range(mp_count):
                yield d, m, d // blocks, m * blocks + d % blocks

    def forward_pairs(r):
        pairs = []
        for d, m, group, source in places():
            target = source ^ r
            to_d = target // parts
            to_m = group * parts + target % parts
            pairs.append((d * mp_count + m, to_d * mp_count + to_m))
        return pairs

    def to_heads(of_round):
        return [
            lax.ppermute(piece, ("dp", "mp"), forward_pairs(r)) for r, piece in enumerate(of_round)
        ]

    def to_blocks(of_round):
        return [
            lax.ppermute(piece, ("dp", "mp"), [(b, a) for a, b in forward_pairs(r)])
            for r, piece in enumerate(of_round)
        ]

    group = dp_count // 2
    own_part = dp_index % group

    def across(array, by):
        return lax.ppermute(array, "dp", [(d, d ^ by) for d in range(dp_count)])

    def with_others(array):
        return [array] + [across(array, r) for r in range(1, group)]

    source_index = mp_index * blocks + dp_index % blocks
    target_index = dp_index * parts + mp_index % parts
    place = jnp.stack([target_index, mp_index, source_index, dp_index, section_index]).astype(jnp.int32)

    met = across(hidden_in, group)
    first_half = dp_index < group
    hidden = jnp.concatenate(
        [jnp.where(first_half, hidden_in, met), jnp.where(first_half, met, hidden_in)], axis=0
    )
    smalls = [w_bcdt[0]] + [across(w_bcdt[0], blocks * r) for r in range(1, dp_count // blocks)]
    gain_share = lax.dynamic_slice_in_dim(norm_gain, mp_index * model_share, model_share, 1)
    table = jnp.concatenate(
        [
            conv_x_weight[0],
            jnp.pad(conv_bc_weight[0], ((0, 0), (0, chan_dev - bc_width))),
            gate_gain,
        ],
        axis=0,
    )
    *held, w, past_x, past_bc, wide, head, now_bc, alive = load(
        slots - dp_index * slots_dev,
        lengths,
        state_pool,
        w_zxo,
        conv_x_pool,
        conv_bc_pool,
        table,
        jnp.concatenate([dt_bias, a_rate, skip_gain], axis=0),
    )

    mine = []
    own = []
    for tick in range(section_count):
        sent = project(
            parts,
            rounds,
            seq_dev,
            blocks,
            small_pad,
            place,
            gain_share,
            w,
            smalls,
            with_others(hidden),
        )
        made = mix(
            tick,
            parts,
            mp_count,
            model_width,
            place,
            past_x,
            past_bc,
            now_bc,
            wide,
            head,
            alive,
            held,
            to_heads(sent),
            mine,
        )
        mine = made[rounds:]
        kept, *others = finish(parts, group, place, w, to_blocks(made[:rounds]))
        total = kept.astype(jnp.float32)
        for r, other in enumerate(others):
            total = total + across(other, r + 1).astype(jnp.float32)
        total = total.astype(jnp.bfloat16)
        hidden, *own = settle(
            tick, group, blocks, chan_total, place, total, across(total, group), hidden, own
        )
        if tick + 1 < section_count:
            swaps = [
                pair
                for a in range(tick % 2, section_count - 1, 2)
                for pair in ((a, a + 1), (a + 1, a))
            ]
            hidden = lax.ppermute(hidden, "section", swaps)
    states = write_states(*mine, held)
    return (own[0][None], states)


def solution(mesh):
    placed = (
        P("dp", "mp"),
        P("dp"),
        P("dp"),
        P("section", None),
        P("section", None, "dp", "mp"),
        P("section", "dp", "mp"),
        P("section", None, "mp"),
        P("section", None, None),
        P("section", "dp", None, "mp"),
        P("section", "dp", None, None),
        P("section", "dp", "mp", None, None),
        P("section", "mp"),
        P("section", "mp"),
        P("section", "mp"),
        P("section", "mp"),
    )
    return jax.shard_map(
        local,
        mesh=mesh,
        in_specs=placed,
        out_specs=(P("section", "dp", "mp"), P("section", "dp", "mp", None, None)),
        check_vma=False,
    )
```

```python
import functools

import jax
import jax.numpy as jnp
from jax import lax
from jax.experimental import pallas as pl
from jax.experimental.pallas import tpu as pltpu
from jax.sharding import PartitionSpec as P

epsilon = 1e-05
LANES = 128
SUBLANES = 8
MEBI = 1 << 20
CHUNKS = 4


def padded(width):
    return -(-width // LANES) * LANES


def in_vmem(count):
    return [pl.BlockSpec(memory_space=pltpu.VMEM)] * count


def in_smem(count):
    return [pl.BlockSpec(memory_space=pltpu.SMEM)] * count


def lanes_of(shape):
    return lax.broadcasted_iota(jnp.int32, shape, 1)


def two_parts(column, lane):
    high = column.astype(jnp.bfloat16).astype(jnp.float32)
    low = column - high
    return jnp.where(lane == 0, high, jnp.where(lane == 1, low, 0.0))


def against(inputs, weights):
    return lax.dot_general(
        inputs, weights, (((1,), (1,)), ((), ())), preferred_element_type=jnp.float32
    )


def load_kernel(
    pieces,
    slots_ref,
    lengths_ref,
    pool_ref,
    w_ref,
    conv_x_ref,
    conv_bc_ref,
    table_ref,
    heads_ref,
    *refs,
):
    held_refs = refs[:CHUNKS]
    (
    w_out_ref,
    past_x_ref,
    past_bc_ref,
    wide_ref,
    head_ref,
    now_bc_ref,
    alive_ref,
    history_x,
    history_bc,
    sems,
    w_sems,
    small_sems,
    ) = refs[CHUNKS:]
    chunk, heads = held_refs[0].shape[:2]
    rows = chunk * CHUNKS
    chan = past_x_ref.shape[1]
    each = heads // pieces

    def copies(c, i):
        for k in range(pieces):
            part = pl.ds(k * each, each)
            yield pltpu.make_async_copy(
                pool_ref.at[0, slots_ref[c * chunk + i], part],
                held_refs[c].at[i, part],
                sems.at[c * chunk + i, k],
            )

    small_copies = [
        pltpu.make_async_copy(source, target, small_sems.at[k])
        for k, (source, target) in enumerate(
            (
                (conv_x_ref, history_x),
                (conv_bc_ref, history_bc),
            )
        )
    ]
    w_copies = [
        pltpu.make_async_copy(w_ref.at[0, k], w_out_ref.at[k], w_sems.at[k])
        for k in range(w_out_ref.shape[0])
    ]
    for copy in small_copies + w_copies:
        copy.start()

    for c in range(CHUNKS):

        def start(i, carry):
            for copy in copies(c, i):
                copy.start()
            return carry

        lax.fori_loop(0, chunk, start, 0)
    for copy in small_copies:
        copy.wait()
    alive = jnp.zeros(alive_ref.shape, jnp.float32)
    row = lax.broadcasted_iota(jnp.int32, alive_ref.shape, 0)
    for i in range(rows):
        length = lengths_ref[i]
        for history_ref, above, past_ref in (
            (history_x, 0, past_x_ref),
            (history_bc, 4, past_bc_ref),
        ):
            history = history_ref[0, slots_ref[i]].astype(jnp.float32)
            taps = history.shape[0]
            tap = lax.broadcasted_iota(jnp.int32, (taps, 1), 0)
            known = (length >= taps - tap).astype(jnp.float32)
            past_ref[i : i + 1, :] = jnp.sum(
                history * known * table_ref[above : above + taps, : history.shape[1]],
                axis=0, keepdims=True
            )
        alive = jnp.where(row == i, (length > 0).astype(jnp.float32), alive)
    alive_ref[...] = alive
    onto = lax.broadcasted_iota(jnp.int32, (heads, chan), 0)
    onto = (onto == lanes_of((heads, chan)) // (chan // heads)).astype(jnp.float32)
    for k in range(3):
        wide = jnp.dot(
            jnp.broadcast_to(heads_ref[k : k + 1, :], (SUBLANES, heads)),
            onto,
            precision=lax.Precision.HIGHEST,
            preferred_element_type=jnp.float32,
        )
        wide_ref[k : k + 1, :] = wide[:1]
    wide_ref[3:4, :] = table_ref[8:9, :]
    wide_ref[4:5, :] = table_ref[3:4, :]
    now_bc_ref[...] = table_ref[7:8, : now_bc_ref.shape[1]]
    head_ref[...] = heads_ref[:2, :]
    for copy in w_copies:
        copy.wait()
    for c in range(CHUNKS):

        def wait(i, carry):
            for copy in copies(c, i):
                copy.wait()
            return carry

        lax.fori_loop(0, chunk, wait, 0)


def load(slots, lengths, pool, w, conv_x, conv_bc, table, by_head):
    rows = slots.shape[0]
    heads, head_size, width = pool.shape[2:]
    pieces = 2 if heads % 2 == 0 else 1
    chan = conv_x.shape[3]
    bc_width = conv_bc.shape[3]
    made = rows * heads * head_size * width * 4 + w.size * 2
    return pl.pallas_call(
        functools.partial(load_kernel, pieces),
        out_shape=[
            *[jax.ShapeDtypeStruct((rows // CHUNKS, heads, head_size, width), jnp.float32)] * CHUNKS,
            jax.ShapeDtypeStruct(w.shape[1:], jnp.bfloat16),
            jax.ShapeDtypeStruct((rows, chan), jnp.float32),
            jax.ShapeDtypeStruct((rows, bc_width), jnp.float32),
            jax.ShapeDtypeStruct((5, chan), jnp.float32),
            jax.ShapeDtypeStruct((2, heads), jnp.float32),
            jax.ShapeDtypeStruct((1, bc_width), jnp.float32),
            jax.ShapeDtypeStruct((rows, LANES), jnp.float32),
        ],
        in_specs=in_smem(2) + [pl.BlockSpec(memory_space=pltpu.HBM)] * 4 + in_vmem(2),
        out_specs=in_vmem(7 + CHUNKS),
        scratch_shapes=[
            pltpu.VMEM(conv_x.shape, conv_x.dtype),
            pltpu.VMEM(conv_bc.shape, conv_bc.dtype),
            pltpu.SemaphoreType.DMA((rows, pieces)),
            pltpu.SemaphoreType.DMA((w.shape[1],)),
            pltpu.SemaphoreType.DMA((2,)),
        ],
        compiler_params=pltpu.CompilerParams(vmem_limit_bytes=5 * MEBI),
        cost_estimate=pl.CostEstimate(
            flops=rows * heads * head_size * width * 16, bytes_accessed=made, transcendentals=0
        ),
        name="load",
    )(slots, lengths, pool, w, conv_x, conv_bc, table, by_head)


def for_each_part(target, parts, act):
    if parts == 1:
        act(0)
        return
    for part in range(parts):
        pl.when(target % parts == part)(functools.partial(act, part))


def row_of(target, parts, group, seq_dev, mine):
    block = target // parts
    return pl.multiple_of((((block % group) ^ mine) * 2 + block // group) * seq_dev, seq_dev)


def project_kernel(
    parts, seq_dev, sharers, group, blocks, place_ref, gain_ref, w_ref, *refs
):
    small_refs = refs[:sharers]
    hidden_refs = refs[sharers : sharers + group]
    *out_refs, scaled_ref, held = refs[sharers + group :]
    chan = w_ref.shape[1]
    piece = chan // parts
    wide = 2 * chan
    source, dp_index = place_ref[2], place_ref[3]
    lane = lanes_of((hidden_refs[0].shape[0], LANES))
    for k, hidden_ref in enumerate(hidden_refs):
        hidden = hidden_ref[...].astype(jnp.float32)
        rows = slice(k * hidden.shape[0], (k + 1) * hidden.shape[0])
        scaled_ref[rows, :] = (hidden * gain_ref[...]).astype(jnp.bfloat16)
        square = jnp.sum(hidden * hidden, axis=1, keepdims=True)
        held[rows, held.shape[1] - LANES :] = two_parts(square, lane).astype(jnp.bfloat16)
    scaled = scaled_ref[...]
    held[:, :chan] = against(scaled, w_ref[1]).astype(jnp.bfloat16)
    held[:, chan:wide] = against(scaled, w_ref[0]).astype(jnp.bfloat16)
    small_width = held.shape[1] - LANES - wide
    tail = jnp.zeros((scaled.shape[0], small_width), jnp.float32)
    for r, small_ref in enumerate(small_refs):
        count = small_ref.shape[0]
        block = ((dp_index // blocks) ^ r) * blocks + dp_index % blocks
        onto = lax.broadcasted_iota(jnp.int32, (count, small_width), 0) + block * count
        onto = (onto == lanes_of((count, small_width))).astype(jnp.bfloat16)
        small = against(scaled, small_ref[...]).astype(jnp.bfloat16)
        tail = tail + jnp.dot(small, onto, preferred_element_type=jnp.float32)
    held[:, wide : wide + small_width] = tail.astype(jnp.bfloat16)
    for r, out_ref in enumerate(out_refs):
        target = source ^ r
        rows = pl.ds(row_of(target, parts, group, seq_dev, dp_index % group), seq_dev)

        def fill(first):
            out_ref[:, :piece] = held[rows, first : first + piece]
            out_ref[:, piece : 2 * piece] = held[rows, chan + first : chan + first + piece]

        for_each_part(target, parts, lambda part: fill(part * piece))
        out_ref[:, 2 * piece :] = held[rows, wide:]


def project(parts, rounds, seq_dev, blocks, small_width, place, gain, w, smalls, hiddens):
    chan, share = w.shape[1:]
    width = 2 * chan // parts + small_width + LANES
    rows = hiddens[0].shape[0] * len(hiddens)
    return pl.pallas_call(
        functools.partial(project_kernel, parts, seq_dev, len(smalls), len(hiddens), blocks),
        out_shape=[jax.ShapeDtypeStruct((seq_dev, width), jnp.bfloat16)] * rounds,
        in_specs=in_smem(1) + in_vmem(2 + len(smalls) + len(hiddens)),
        out_specs=in_vmem(rounds),
        scratch_shapes=[
            pltpu.VMEM((rows, share), jnp.bfloat16),
            pltpu.VMEM((rows, 2 * chan + small_width + LANES), jnp.bfloat16),
        ],
        compiler_params=pltpu.CompilerParams(vmem_limit_bytes=6 * MEBI),
        cost_estimate=pl.CostEstimate(
            flops=2 * rows * share * (2 * chan + small_width),
            bytes_accessed=2 * share * (2 * chan + small_width),
            transcendentals=0,
        ),
        name="project",
    )(place, gain, w, *smalls, *hiddens)


def mix_kernel(
    tick,
    rounds,
    parts,
    mp_count,
    model_width,
    heads,
    place_ref,
    past_x_ref,
    past_bc_ref,
    now_bc_ref,
    wide_ref,
    head_ref,
    alive_ref,
    *refs,
):
    held_refs = refs[:CHUNKS]
    refs = refs[CHUNKS:]
    got_refs = refs[:rounds]
    before_refs = refs[rounds : rounds + 3 * (tick > 0)]
    refs = refs[rounds + len(before_refs) :]
    out_refs = refs[:rounds]
    decay_ref, x_ref, b_ref, c_ref, read_ref, gated_ref, inner_ref, gate_ref = refs[rounds:]

    def keep(k, ref, value):
        if tick > 0:
            value = jnp.where(place_ref[4] == tick, value, before_refs[k][...])
        ref[...] = value

    seq_dev, chan = past_x_ref.shape
    head_size = chan // heads
    bc_width = past_bc_ref.shape[1]
    blocks = max(1, rounds // mp_count)
    piece = chan // blocks
    target = place_ref[0]
    mp_index = place_ref[1]
    tail_width = got_refs[0].shape[1] - 2 * piece

    for j in range(blocks):
        both = jnp.zeros((seq_dev, 2 * piece), jnp.float32)
        for r, got_ref in enumerate(got_refs):
            chosen = ((target ^ r) % blocks == j).astype(jnp.float32)
            both = both + chosen * got_ref[:, : 2 * piece].astype(jnp.float32)
        inner_ref[:, j * piece : (j + 1) * piece] = both[:, :piece]
        gate_ref[:, j * piece : (j + 1) * piece] = both[:, piece:]
    tail = jnp.zeros((seq_dev, tail_width), jnp.float32)
    for got_ref in got_refs:
        tail = tail + got_ref[:, 2 * piece :].astype(jnp.float32)
    square = jnp.sum(tail[:, tail_width - LANES :], axis=1, keepdims=True) / blocks
    scale = lax.rsqrt(square / model_width + epsilon)
    conv_bc = jax.nn.silu(past_bc_ref[...] + tail[:, :bc_width] * scale * now_bc_ref[...])
    conv_b = conv_bc[:, : bc_width // 2]
    conv_c = conv_bc[:, bc_width // 2 :]
    keep(2, b_ref, conv_b)
    c_ref[...] = conv_c
    read_ref[...] = jnp.zeros_like(read_ref)
    group = min(heads, 8)
    while group and (heads % group or group * head_size % LANES):
        group -= 1
    group = group or heads

    chunk = seq_dev // CHUNKS
    several = heads // group
    whole_tiles = group * head_size % LANES == 0
    lane_groups = {k for k in range(several) if k % 5 in (1, 3)} if whole_tiles else set()

    def lane_sums(values):
        return jnp.sum(values.T, axis=0, keepdims=True)

    def work(c, at, carry):
        i = c * chunk + at
        c_row = c_ref[pl.ds(i, 1), :]
        c_rows = jnp.broadcast_to(c_row, (SUBLANES, conv_c.shape[1]))
        c_rows = c_rows.astype(jnp.bfloat16)
        found = []
        for first in range(0, heads, group):
            state = held_refs[c][at, first : first + group]
            state = state.reshape(group * head_size, state.shape[2])
            if first // group in lane_groups:
                found.append(
                    jnp.concatenate(
                        [
                            lane_sums(state[k : k + LANES] * c_row)
                            for k in range(0, group * head_size, LANES)
                        ],
                        axis=1,
                    )
                )
            else:
                found.append(against(c_rows, state.astype(jnp.bfloat16)))
        tile = pl.ds(pl.multiple_of(i // SUBLANES * SUBLANES, SUBLANES), SUBLANES)
        width = group * head_size
        mine = lax.broadcasted_iota(jnp.int32, (SUBLANES, width), 0) == i % SUBLANES
        for k, y in enumerate(found):
            columns = slice(k * width, (k + 1) * width)
            read_ref[tile, columns] = jnp.where(mine, y, read_ref[tile, columns])
        return carry

    for c in range(CHUNKS):
        lax.fori_loop(0, chunk, functools.partial(work, c), 0)

    raw = tail[:, bc_width : tail_width - LANES] * scale
    raw_width = raw.shape[1]
    pick = lambda shape, per: (
        lax.broadcasted_iota(jnp.int32, shape, 0) == mp_index * heads + lanes_of(shape) // per
    ).astype(jnp.float32)
    chosen = lambda per, width: jnp.dot(
        raw,
        pick((raw_width, width), per),
        precision=lax.Precision.HIGHEST,
        preferred_element_type=jnp.float32,
    )
    softplus = lambda v: jnp.maximum(v, 0.0) + jnp.log1p(jnp.exp(-jnp.abs(v)))
    alive = alive_ref[:, :1]
    step_heads = softplus(chosen(1, heads) + head_ref[0:1, :])
    keep(0, decay_ref, jnp.exp(-step_heads * head_ref[1:2, :]) * alive)
    step = softplus(chosen(head_size, chan) + wide_ref[0:1, :])
    decay = jnp.exp(-step * wide_ref[1:2, :]) * alive
    conv_x = jax.nn.silu(past_x_ref[...] + inner_ref[...] * scale * wide_ref[4:5, :])
    x_step = conv_x * step
    keep(1, x_ref, x_step)
    cross = jnp.sum(conv_b * conv_c, axis=1, keepdims=True)
    y = decay * read_ref[...] + x_step * cross + wide_ref[2:3, :] * conv_x
    gated = y * jax.nn.silu(gate_ref[...] * scale)
    square = jnp.sum(gated * gated, axis=1, keepdims=True)
    gated_ref[...] = (gated * wide_ref[3:4, :]).astype(jnp.bfloat16)
    out_tail = two_parts(square, lanes_of((seq_dev, LANES))).astype(jnp.bfloat16)
    for r, out_ref in enumerate(out_refs):
        first = pl.multiple_of((target ^ r) % blocks * piece, LANES) if blocks > 1 else 0
        out_ref[:, :piece] = gated_ref[:, pl.ds(first, piece)]
        out_ref[:, piece:] = out_tail


def mix(
    tick, parts, mp_count, model_width, place, past_x, past_bc, now_bc, wide, head, alive, held,
    got, before,
):
    rounds = len(got)
    seq_dev, chan = past_x.shape
    heads = head.shape[1]
    piece = chan // max(1, rounds // mp_count)
    state_size = held[0].shape[3]
    return pl.pallas_call(
        functools.partial(mix_kernel, tick, rounds, parts, mp_count, model_width, heads),
        out_shape=[jax.ShapeDtypeStruct((seq_dev, piece + LANES), jnp.bfloat16)] * rounds
        + [
            jax.ShapeDtypeStruct((seq_dev, heads), jnp.float32),
            jax.ShapeDtypeStruct((seq_dev, chan), jnp.float32),
            jax.ShapeDtypeStruct((seq_dev, state_size), jnp.float32),
        ],
        in_specs=in_smem(1) + in_vmem(6 + CHUNKS + rounds + len(before)),
        out_specs=in_vmem(rounds + 3),
        scratch_shapes=[
            pltpu.VMEM((seq_dev, state_size), jnp.float32),
            pltpu.VMEM((seq_dev, chan), jnp.float32),
            pltpu.VMEM((seq_dev, chan), jnp.bfloat16),
            pltpu.VMEM((seq_dev, chan), jnp.float32),
            pltpu.VMEM((seq_dev, chan), jnp.float32),
        ],
        compiler_params=pltpu.CompilerParams(vmem_limit_bytes=10 * MEBI),
        cost_estimate=pl.CostEstimate(
            flops=16 * seq_dev * chan * state_size,
            bytes_accessed=seq_dev * chan * state_size * 4,
            transcendentals=0,
        ),
        name="mix",
    )(place, past_x, past_bc, now_bc, wide, head, alive, *held, *got, *before)


def finish_kernel(rounds, parts, seq_dev, group, place_ref, w_ref, *refs):
    got_refs = refs[:rounds]
    out_refs = refs[rounds : rounds + group]
    rows_ref, square_ref = refs[rounds + group :]
    piece = got_refs[0].shape[1] - LANES
    square_ref[...] = jnp.zeros_like(square_ref)
    for r, got_ref in enumerate(got_refs):
        target = place_ref[2] ^ r
        rows = pl.ds(row_of(target, parts, group, seq_dev, place_ref[3] % group), seq_dev)

        def fill(first):
            rows_ref[rows, first : first + piece] = got_ref[:, :piece]

        for_each_part(target, parts, lambda part: fill(part * piece))
        square_ref[rows, :] += got_ref[:, piece:].astype(jnp.float32)
    square = jnp.sum(square_ref[...], axis=1, keepdims=True)
    tail = two_parts(square, lanes_of(square_ref.shape)).astype(jnp.bfloat16)
    partial = jnp.dot(rows_ref[...], w_ref[2], preferred_element_type=jnp.float32)
    partial = partial.astype(jnp.bfloat16)
    for k, out_ref in enumerate(out_refs):
        rows = slice(2 * seq_dev * k, 2 * seq_dev * (k + 1))
        out_ref[:, :LANES] = tail[rows]
        out_ref[:, LANES:] = partial[rows]


def finish(parts, group, place, w, got):
    rounds = len(got)
    chan, share = w.shape[1:]
    seq_dev = got[0].shape[0]
    seq_all = 2 * seq_dev * group
    return pl.pallas_call(
        functools.partial(finish_kernel, rounds, parts, seq_dev, group),
        out_shape=[jax.ShapeDtypeStruct((2 * seq_dev, LANES + share), jnp.bfloat16)] * group,
        in_specs=in_smem(1) + in_vmem(1 + rounds),
        out_specs=in_vmem(group),
        scratch_shapes=[
            pltpu.VMEM((seq_all, chan), jnp.bfloat16),
            pltpu.VMEM((seq_all, LANES), jnp.float32),
        ],
        compiler_params=pltpu.CompilerParams(vmem_limit_bytes=6 * MEBI),
        cost_estimate=pl.CostEstimate(
            flops=2 * seq_all * chan * share, bytes_accessed=2 * chan * share, transcendentals=0
        ),
        name="finish",
    )(place, w, *got)


def settle_kernel(tick, seq_dev, group, blocks, chan_total, place_ref, mine_ref, met_ref, old_ref, *refs):
    *before_refs, hidden_ref, own_ref = refs
    total = mine_ref[...].astype(jnp.float32) + met_ref[...].astype(jnp.float32)
    square = jnp.sum(total[:, :LANES], axis=1, keepdims=True) / blocks
    scale = lax.rsqrt(square / chan_total + epsilon)
    hidden = old_ref[...].astype(jnp.float32) + total[:, LANES:] * scale
    hidden_ref[...] = hidden.astype(jnp.bfloat16)
    first = pl.multiple_of(place_ref[3] // group * seq_dev, seq_dev)
    own = hidden_ref[pl.ds(first, seq_dev), :]
    for before_ref in before_refs:
        own = jnp.where(place_ref[4] == tick, own, before_ref[...])
    own_ref[...] = own


def settle(tick, group, blocks, chan_total, place, mine, met, old, before):
    rows, share = old.shape
    return pl.pallas_call(
        functools.partial(settle_kernel, tick, rows // 2, group, blocks, chan_total),
        out_shape=[
            jax.ShapeDtypeStruct((rows, share), jnp.bfloat16),
            jax.ShapeDtypeStruct((rows // 2, share), jnp.bfloat16),
        ],
        in_specs=in_smem(1) + in_vmem(3 + len(before)),
        out_specs=in_vmem(2),
        compiler_params=pltpu.CompilerParams(vmem_limit_bytes=4 * MEBI),
        cost_estimate=pl.CostEstimate(flops=rows * share * 8, bytes_accessed=rows * share * 10, transcendentals=0),
        name="settle",
    )(place, mine, met, old, *before)


def write_kernel(decay_ref, x_ref, b_ref, *refs):
    states_refs = refs[:CHUNKS]
    out_ref, held, sems = refs[CHUNKS:]
    rows, heads, head_size, width = held.shape
    together = LANES // head_size

    def copy_out(i):
        return pltpu.make_async_copy(held.at[i], out_ref.at[0, i], sems.at[i])

    chunk = rows // CHUNKS

    def work(c, at, carry):
        i = c * chunk + at
        b_rows = jnp.broadcast_to(b_ref[pl.ds(i, 1), :], (LANES, width))
        tile = pl.ds(pl.multiple_of(i // SUBLANES * SUBLANES, SUBLANES), SUBLANES)
        for first in range(0, heads, together):
            count = min(together, heads - first)
            columns = slice(first * head_size, (first + count) * head_size)
            chosen = lax.broadcasted_iota(jnp.int32, (SUBLANES, count * head_size), 0) == i % SUBLANES
            x_row = jnp.sum(jnp.where(chosen, x_ref[tile, columns], 0.0), axis=0, keepdims=True)
            x_rows = jnp.broadcast_to(x_row, (LANES, count * head_size))
            added = x_rows.T * b_rows[: count * head_size]
            for k in range(count):
                held[i, first + k] = (
                    states_refs[c][at, first + k] * decay_ref[i, first + k]
                    + added[k * head_size : (k + 1) * head_size]
                )
        copy_out(i).start()
        return carry

    def end(i, carry):
        copy_out(i).wait()
        return carry

    for c in range(CHUNKS):
        lax.fori_loop(0, chunk, functools.partial(work, c), 0)
    lax.fori_loop(0, rows, end, 0)


def write_states(decay, x, b, states):
    chunk, heads, head_size, width = states[0].shape
    rows = chunk * len(states)
    return pl.pallas_call(
        write_kernel,
        out_shape=jax.ShapeDtypeStruct((1, rows, heads, head_size, width), jnp.float32),
        in_specs=in_smem(1) + in_vmem(2 + CHUNKS),
        out_specs=pl.BlockSpec(memory_space=pl.ANY),
        scratch_shapes=[
            pltpu.VMEM((rows, heads, head_size, width), jnp.float32),
            pltpu.SemaphoreType.DMA((rows,)),
        ],
        compiler_params=pltpu.CompilerParams(
            vmem_limit_bytes=rows * heads * head_size * width * 4 + 3 * MEBI
        ),
        cost_estimate=pl.CostEstimate(
            flops=16 * rows * heads * head_size * width,
            bytes_accessed=rows * heads * head_size * width * 8,
            transcendentals=0,
        ),
        name="write_states",
    )(decay, x, b, *states)


def local(
    hidden_in,
    lengths,
    slots,
    norm_gain,
    w_zxo,
    w_bcdt,
    conv_x_weight,
    conv_bc_weight,
    conv_x_pool,
    conv_bc_pool,
    state_pool,
    a_rate,
    dt_bias,
    skip_gain,
    gate_gain,
):
    section_index = lax.axis_index("section")
    section_count = lax.axis_size("section")
    mp_index = lax.axis_index("mp")
    mp_count = lax.axis_size("mp")
    dp_index = lax.axis_index("dp")
    dp_count = lax.axis_size("dp")
    seq_dev, model_share = hidden_in.shape
    seq_all = seq_dev * dp_count
    model_width = norm_gain.shape[1]
    heads_dev = a_rate.shape[1]
    head_size = state_pool.shape[3]
    chan_dev = heads_dev * head_size
    slots_dev = state_pool.shape[1]
    bc_width = conv_bc_weight.shape[2]
    small_dev = w_bcdt.shape[1]
    small_all = small_dev * dp_count
    chan_saved = w_zxo.shape[2]
    chan_total = chan_saved * dp_count
    small_pad = bc_width + padded(small_all - bc_width)

    blocks = max(1, dp_count // mp_count)
    parts = max(1, mp_count // dp_count)
    rounds = dp_count * parts

    def places():
        for d in range(dp_count):
            for m in range(mp_count):
                yield d, m, d // blocks, m * blocks + d % blocks

    def forward_pairs(r):
        pairs = []
        for d, m, group, source in places():
            target = source ^ r
            to_d = target // parts
            to_m = group * parts + target % parts
            pairs.append((d * mp_count + m, to_d * mp_count + to_m))
        return pairs

    def to_heads(of_round):
        return [
            lax.ppermute(piece, ("dp", "mp"), forward_pairs(r)) for r, piece in enumerate(of_round)
        ]

    def to_blocks(of_round):
        return [
            lax.ppermute(piece, ("dp", "mp"), [(b, a) for a, b in forward_pairs(r)])
            for r, piece in enumerate(of_round)
        ]

    group = dp_count // 2
    own_part = dp_index % group

    def across(array, by):
        return lax.ppermute(array, "dp", [(d, d ^ by) for d in range(dp_count)])

    def with_others(array):
        return [array] + [across(array, r) for r in range(1, group)]

    source_index = mp_index * blocks + dp_index % blocks
    target_index = dp_index * parts + mp_index % parts
    place = jnp.stack([target_index, mp_index, source_index, dp_index, section_index]).astype(jnp.int32)

    met = across(hidden_in, group)
    smalls = [w_bcdt[0]] + [across(w_bcdt[0], blocks * r) for r in range(1, dp_count // blocks)]
    gain_share = lax.dynamic_slice_in_dim(norm_gain, mp_index * model_share, model_share, 1)
    table = jnp.concatenate(
        [
            conv_x_weight[0],
            jnp.pad(conv_bc_weight[0], ((0, 0), (0, chan_dev - bc_width))),
            gate_gain,
        ],
        axis=0,
    )
    first_half = jnp.broadcast_to(dp_index < group, (seq_dev, model_share))
    place, gain_share, first_half, local_slots = lax.optimization_barrier(
        (place, gain_share, first_half, slots - dp_index * slots_dev)
    )
    *held, w, past_x, past_bc, wide, head, now_bc, alive = load(
        local_slots,
        lengths,
        state_pool,
        w_zxo,
        conv_x_pool,
        conv_bc_pool,
        table,
        jnp.concatenate([dt_bias, a_rate, skip_gain], axis=0),
    )

    met, alive = lax.optimization_barrier((met, alive))
    hidden = jnp.concatenate(
        [jnp.where(first_half, hidden_in, met), jnp.where(first_half, met, hidden_in)], axis=0
    )
    mine = []
    own = []
    for tick in range(section_count):
        sent = project(
            parts,
            rounds,
            seq_dev,
            blocks,
            small_pad,
            place,
            gain_share,
            w,
            smalls,
            with_others(hidden),
        )
        made = mix(
            tick,
            parts,
            mp_count,
            model_width,
            place,
            past_x,
            past_bc,
            now_bc,
            wide,
            head,
            alive,
            held,
            to_heads(sent),
            mine,
        )
        mine = made[rounds:]
        kept, *others = finish(parts, group, place, w, to_blocks(made[:rounds]))
        total = kept.astype(jnp.float32)
        for r, other in enumerate(others):
            total = total + across(other, r + 1).astype(jnp.float32)
        total = total.astype(jnp.bfloat16)
        hidden, *own = settle(
            tick, group, blocks, chan_total, place, total, across(total, group), hidden, own
        )
        if tick + 1 < section_count:
            swaps = [
                pair
                for a in range(tick % 2, section_count - 1, 2)
                for pair in ((a, a + 1), (a + 1, a))
            ]
            hidden = lax.ppermute(hidden, "section", swaps)
    states = write_states(*mine, held)
    return (own[0][None], states)


def solution(mesh):
    placed = (
        P("dp", "mp"),
        P("dp"),
        P("dp"),
        P("section", None),
        P("section", None, "dp", "mp"),
        P("section", "dp", "mp"),
        P("section", None, "mp"),
        P("section", None, None),
        P("section", "dp", None, "mp"),
        P("section", "dp", None, None),
        P("section", "dp", "mp", None, None),
        P("section", "mp"),
        P("section", "mp"),
        P("section", "mp"),
        P("section", "mp"),
    )
    return jax.shard_map(
        local,
        mesh=mesh,
        in_specs=placed,
        out_specs=(P("section", "dp", "mp"), P("section", "dp", "mp", None, None)),
        check_vma=False,
    )
```
